32 devices in a mesh: gx: 4 (over z), gy: 8 (over y, x, core).
Axes of the slice: x: 2, y: 2, z: 4, core: 2. Of those that a mesh axis runs over, the one named last changes fastest.
Arguments:
- matrix_rows: float32 [4096, 1024], P(('gx', 'gy')), may hold values from -1.1 to 1.1
- tile_owner: int32 [136], replicated, may hold values from 0 to 31, as said below
- tile_slot: int32 [136], replicated, may hold values from 0 to 4, as said below
Outputs:
- packed_tiles: float32 [160, 256, 256], P(('gx', 'gy'))
The draws below stay inside these ranges and needn't reach their ends.
Inputs may be any that keep to these rules, and one draw needn't show every extreme that they name: `tile_owner`: give tile (I, J) the class (c, r) as follows, with a = I // 4, b = J // 4, i = I % 4, j = J % 4: if a == b, c = a and r = i when i - j < 2, else r = j; if a > b and (a - b > 2, or a - b == 2 with i + j even), c = b and r = i; otherwise c = a and r = j. The owner of a class (c, r) tile is one of the devices c * 8 to c * 8 + 7. Every owner holds 4 or 5 tiles. At most 2 tiles of one class share an owner, and in every draw some owner holds exactly 2 tiles of one class. `tile_slot`: the tiles of one owner take the slots 0 to their count - 1, each once.
All inputs are finite; a program needn't handle non-finite values.
Results may differ from the reference program's by a relative error of at most 0.0003.
Values sent between devices are 32-bit elements; how exact they have to be, the bound alone decides.
A program may use at most 128 MiB of HBM per device.

```python
import jax
import jax.numpy as jnp
import numpy as np
from jax import lax

WIDTH = 1024
TILE = 256
ORDER = 4096
TILE_COUNT = 16
HALF_TILES = 4
LOWER_COUNT = 136
SLOTS = 5
N_GX = 4
N_GY = 8
DEVICES = 32


def tile_classes():
    lower_i, lower_j = np.tril_indices(TILE_COUNT)
    group_a = lower_i // HALF_TILES
    group_b = lower_j // HALF_TILES
    inner_i = lower_i % HALF_TILES
    inner_j = lower_j % HALF_TILES
    same = group_a == group_b
    within_row = inner_i - inner_j < HALF_TILES // 2
    gap = group_a - group_b
    across_row = (gap > N_GX // 2) | (gap == N_GX // 2) & ((inner_i + inner_j) % 2 == 0)
    rowwise = np.where(same, within_row, across_row)
    class_x = np.where(same | ~rowwise, group_a, group_b)
    class_r = np.where(rowwise, inner_i, inner_j)
    return (class_x.astype(np.int32), class_r.astype(np.int32))


def owner_table(key):
    class_x, class_r = tile_classes()
    set_id = jnp.asarray(class_x * HALF_TILES + class_r, jnp.int32)
    row_of = jnp.asarray(class_x, jnp.int32)
    set_rank = jax.random.permutation(jax.random.fold_in(key, 11), TILE_COUNT).astype(jnp.int32)
    tile_rank = jax.random.permutation(jax.random.fold_in(key, 12), LOWER_COUNT).astype(jnp.int32)
    score = (row_of * TILE_COUNT + set_rank[set_id]) * LOWER_COUNT + tile_rank
    order = jnp.argsort(score, stable=True).astype(jnp.int32)
    position = jnp.zeros((LOWER_COUNT,), jnp.int32).at[order].set(jnp.arange(LOWER_COUNT, dtype=jnp.int32))
    per_row = LOWER_COUNT // N_GX
    inside_row = position % per_row
    row_keys = jax.random.split(jax.random.fold_in(key, 13), N_GX)
    owner_order = jax.vmap(lambda one: jax.random.permutation(one, N_GY))(row_keys).astype(jnp.int32)
    owners = row_of * N_GY + owner_order[row_of, inside_row % N_GY]
    slot_index = inside_row // N_GY
    return (owners.astype(jnp.int32), slot_index.astype(jnp.int32))


def draw_tile_owner(key, part):
    return owner_table(key)[0]


def draw_tile_slot(key, part):
    return owner_table(key)[1]


def shard_levels(own_key, dims, shards, smallest, largest):
    def one(dim, shards_of):
        heights = jax.random.uniform(jax.random.fold_in(jax.random.fold_in(own_key, 6), dim), (shards_of,), jnp.float32, smallest / len(shards), largest / len(shards))
        return jnp.repeat(jnp.exp(heights), dims[dim] // shards_of).reshape((-1,) + (1,) * (len(dims) - dim - 1))

    level = one(*shards[0])
    for cut in shards[1:]:
        level = level * one(*cut)
    return level


def normal_values(stream_key, extent, width, limit, pieces=(), kind=jnp.bfloat16):
    gain = shard_levels(stream_key, extent, pieces, -0.22, 0.18) if pieces else 1.0
    values = jax.random.normal(stream_key, extent, jnp.float32) * width * gain
    return jnp.minimum(jnp.maximum(values, -limit), limit).astype(kind)


def setup_inputs(seed: int = 0) -> dict:
    splits = jax.random.split(jax.random.key(seed), 4)
    matrix_rows = normal_values(splits[0], (ORDER, WIDTH), 0.177, 1.1, ((0, 32),), jnp.float32)
    tile_owner = draw_tile_owner(jax.random.fold_in(splits[3], 71), 0)
    tile_slot = draw_tile_slot(jax.random.fold_in(splits[3], 71), 0)
    return dict(matrix_rows=matrix_rows, tile_owner=tile_owner, tile_slot=tile_slot)


def reference(matrix_rows, tile_owner, tile_slot):
    lower_i, lower_j = np.tril_indices(TILE_COUNT)
    row_table = jnp.asarray(lower_i, jnp.int32)
    col_table = jnp.asarray(lower_j, jnp.int32)
    blocks = matrix_rows.reshape(TILE_COUNT, TILE, WIDTH)
    inside = lax.broadcasted_iota(jnp.int32, (TILE, TILE), 0)
    across = lax.broadcasted_iota(jnp.int32, (TILE, TILE), 1)

    def one_tile(index):
        row_tile = row_table[index]
        col_tile = col_table[index]
        product = lax.dot_general(blocks[row_tile], blocks[col_tile], (((1,), (1,)), ((), ())),
                                  precision=lax.Precision.HIGHEST, preferred_element_type=jnp.float32)
        upper = jnp.logical_and(row_tile == col_tile, inside < across)
        return jnp.where(upper, jnp.float32(0.0), product)

    tiles = lax.map(one_tile, jnp.arange(LOWER_COUNT, dtype=jnp.int32))
    packed = jnp.zeros((DEVICES, SLOTS, TILE, TILE), jnp.float32)
    packed = packed.at[tile_owner, tile_slot].set(tiles)
    return packed.reshape(DEVICES * SLOTS, TILE, TILE)
```

```python
import functools

import jax
import jax.numpy as jnp
from jax import lax
from jax.experimental import pallas as pl
from jax.experimental.pallas import tpu as pltpu
from jax.sharding import PartitionSpec as P

MESH = pl.DeviceIdType.MESH


def chip_position(chip, chips):
    row, col = lax.div(chip, 2), lax.rem(chip, 2)
    return col * (1 + row) + (1 - col) * lax.rem(chips - row, chips)


def chip_at(position, chips):
    behind = lax.rem(position + chips - 1, chips)
    far = lax.div(behind, chips // 2)
    return (1 - far) * (2 * behind + 1) + far * 2 * (chips - 1 - behind)


def piece_lists(half_tiles, half_x):
    lists, start = [], 0
    for step in range(half_x + 1):
        if step == 0:
            count = half_tiles // 2 + 1
        elif step < half_x:
            count = half_tiles
        else:
            count = half_tiles // 2
        lists.append((step, start, count))
        start += count
    return lists, start


def piece(x, r, step, i, nx, half_tiles, half_x):
    source = lax.rem(x - step + nx, nx)
    if step == 0:
        col = lax.rem(r - i + half_tiles, half_tiles)
        valid = jnp.logical_or(i < half_tiles // 2, r < half_tiles // 2)
        rowwise = col <= r
    elif step < half_x:
        col = i
        valid = i >= 0
        rowwise = source > x
    else:
        flag = jnp.where(x >= half_x, 1, 0)
        col = 2 * i + lax.rem(r + flag, 2)
        valid = i >= 0
        rowwise = source > x
    other, mine = source * half_tiles + r, x * half_tiles + col
    row_tile = jnp.where(rowwise, other, mine)
    col_tile = jnp.where(rowwise, mine, other)
    tile = jnp.where(valid, row_tile * (row_tile + 1) // 2 + col_tile, 0)
    return col, valid, rowwise, tile


def kernel(
    dims, rows_ref, owner_ref, slot_ref, out_ref,
    gath, zbuf, chi, clo, zhi, zlo, pieces, outgoing, incoming, targets,
    gs_r, gr_r, gs_l, gr_l, ss, sr, zs, zr, xs, xr,
):
    nx, ny, half_tiles, half_x, capacity, slots = dims
    rows = rows_ref.shape[0]
    half = rows // 2
    chips = ny // 2
    reach = chips // 2
    x = lax.axis_index("gx")
    y = lax.axis_index("gy")
    core = lax.rem(y, 2)
    chip = lax.div(y, 2)
    right_x, left_x = lax.rem(x + 1, nx), lax.rem(x + nx - 1, nx)
    sibling = y + 1 - 2 * core
    place = chip_position(chip, chips)

    def at(position):
        return 2 * chip_at(lax.rem(position + chips, chips), chips) + core

    next_y, prev_y = at(place + 1), at(place - 1)
    lists, piece_count = piece_lists(half_tiles, half_x)

    barrier = pltpu.get_barrier_semaphore()
    for other in (right_x, left_x):
        pl.semaphore_signal(barrier, inc=1, device_id=(other, y), device_id_type=MESH)
    for offset in range(1, ny):
        pl.semaphore_signal(
            barrier, inc=1, device_id=(x, lax.rem(y + offset, ny)), device_id_type=MESH
        )
    pl.semaphore_wait(barrier, ny + 1)

    started = []

    def send(src, dst, send_sem, recv_sem, target):
        copy = pltpu.make_async_remote_copy(
            src_ref=src, dst_ref=dst, send_sem=send_sem, recv_sem=recv_sem,
            device_id=target, device_id_type=MESH,
        )
        copy.start()
        started.append(copy)

    def part(h):
        return pl.ds(h * half, half)

    def zcopy(step, h):
        src = rows_ref.at[part(h)] if step == 1 else zbuf.at[step - 2, part(h)]
        send(src, zbuf.at[step - 1, part(h)], zs.at[step - 1, h], zr.at[step - 1, h], (right_x, y))

    def block(owner, h):
        return gath.at[owner, part(h)]

    def ring(direction, distance, h):
        owner = at(place - direction * (distance - 1))
        src = rows_ref.at[part(h)] if distance == 1 else block(owner, h)
        s, r = (gs_r, gr_r) if direction == 1 else (gs_l, gr_l)
        target = next_y if direction == 1 else prev_y
        send(src, block(owner, h), s.at[distance - 1, h], r.at[distance - 1, h], (x, target))

    def cross(number, owner, h):
        src = rows_ref.at[part(h)] if number == 0 else block(owner, h)
        send(src, block(owner, h), ss.at[number, h], sr.at[number, h], (x, sibling))

    def halves_of(direction, distance):
        if distance < reach:
            return (0, 1) if direction == 1 else (1, 0)
        return (0,) if direction == 1 else (1,)

    def split(value, hi_ref, lo_ref, index):
        hi = value.astype(jnp.bfloat16)
        hi_ref[index] = hi
        lo_ref[index] = (value - hi.astype(jnp.float32)).astype(jnp.bfloat16)

    zcopy(1, 0)
    ring(1, 1, 0)
    if reach > 1:
        ring(-1, 1, 1)
        zcopy(1, 1)
        ring(1, 1, 1)
        ring(-1, 1, 0)
    else:
        ring(-1, 1, 1)
        zcopy(1, 1)
    cross(0, y, 0)
    cross(0, y, 1)

    for step, first, count in lists:
        def fill(i, carry, step=step, first=first):
            _, valid, _, tile = piece(x, chip, step, i, nx, half_tiles, half_x)
            targets[first + i] = jnp.where(valid, lax.rem(owner_ref[tile], ny), ny)
            return carry
        lax.fori_loop(0, count, fill, 0)

    me = x * ny + y

    def class_loop(r, carry):
        state = (jnp.int32(0),) + carry
        for step, first, count in lists:
            def look(i, state, step=step):
                seen, found = state[0], state[1:]
                _, valid, rowwise, tile = piece(x, r, step, i, nx, half_tiles, half_x)
                mine = jnp.where(valid, jnp.where(owner_ref[tile] == me, 1, 0), 0)
                slot = slot_ref[tile]
                code = 2 * (r * capacity + jnp.minimum(seen, capacity - 1))
                code = code + jnp.where(rowwise, 1, 0)
                key = jnp.where(mine == 1, slot, slots)
                found = tuple(jnp.where(key == s, code, found[s]) for s in range(slots))
                return (seen + mine,) + found
            state = lax.fori_loop(0, count, look, state)
        return state[1:]

    found = lax.fori_loop(0, half_tiles, class_loop, (jnp.int32(-1),) * slots)

    chosen = []
    for offset in range(ny):
        dest = lax.rem(y + offset, ny)

        def pick(p, state, dest=dest):
            hit = jnp.where(targets[p] == dest, 1, 0)
            seen = state[0]
            key = jnp.where(hit == 1, seen, capacity)
            picks = tuple(jnp.where(key == k, p, state[1 + k]) for k in range(capacity))
            return (seen + hit,) + picks

        chosen.append(lax.fori_loop(0, piece_count, pick, (jnp.int32(0),) * (capacity + 1))[1:])

    def wait_recv(dst, sem):
        pltpu.make_async_remote_copy(
            src_ref=dst, dst_ref=dst, send_sem=sem, recv_sem=sem,
            device_id=(x, sibling), device_id_type=MESH,
        ).wait_recv()

    split(rows_ref[...], zhi, zlo, 0)
    split(rows_ref[...], chi, clo, y)

    def take_cross(number, owner, halves):
        for h in halves:
            wait_recv(block(owner, h), sr.at[number, h])

    number = 1
    pending = [(0, sibling, (0, 1))]
    for distance in range(1, reach + 1):
        if distance <= half_x:
            for h in (0, 1):
                wait_recv(zbuf.at[distance - 1, part(h)], zr.at[distance - 1, h])
                if distance < half_x:
                    zcopy(distance + 1, h)
                if h in halves_of(1, distance):
                    owner = at(place - distance)
                    wait_recv(block(owner, h), gr_r.at[distance - 1, h])
                    if distance < reach and h in halves_of(1, distance + 1):
                        ring(1, distance + 1, h)
                    cross(2 * distance - 1, owner, h)
                g = 1 - h
                if g in halves_of(-1, distance):
                    owner = at(place + distance)
                    wait_recv(block(owner, g), gr_l.at[distance - 1, g])
                    if distance < reach and g in halves_of(-1, distance + 1):
                        ring(-1, distance + 1, g)
                    cross(2 * distance, owner, g)
            split(zbuf[distance - 1], zhi, zlo, distance)
        behind, ahead = at(place - distance), at(place + distance)
        pending.append((2 * distance - 1, behind + 1 - 2 * core, halves_of(1, distance)))
        pending.append((2 * distance, ahead + 1 - 2 * core, halves_of(-1, distance)))
        split(gath[behind], chi, clo, behind)
        if distance < reach:
            split(gath[ahead], chi, clo, ahead)
        for number, owner, halves in pending[: (1 if distance == 1 else 0)]:
            take_cross(number, owner, halves)
            split(gath[owner], chi, clo, owner)
    for number, owner, halves in pending[1:-2]:
        take_cross(number, owner, halves)
        split(gath[owner], chi, clo, owner)
    for number, owner, halves in pending[-2:]:
        take_cross(number, owner, halves)
    split(gath[pending[-1][1]], chi, clo, pending[-1][1])
    for step in range(reach + 1, half_x + 1):
        for h in (0, 1):
            wait_recv(zbuf.at[step - 1, part(h)], zr.at[step - 1, h])
            if step < half_x:
                zcopy(step + 1, h)
        split(zbuf[step - 1], zhi, zlo, step)

    def mul(a_hi, a_lo, b_hi, b_lo):
        dims_nt = (((1,), (1,)), ((), ()))
        one = functools.partial(
            lax.dot_general, dimension_numbers=dims_nt, preferred_element_type=jnp.float32
        )
        return one(a_hi, b_hi) + (one(a_hi, b_lo) + one(a_lo, b_hi))

    width = rows_ref.shape[1]
    row_inside = core * rows + lax.broadcasted_iota(jnp.int32, (rows, 2 * rows), 0)
    col_inside = lax.broadcasted_iota(jnp.int32, (rows, 2 * rows), 1)
    above = jnp.where(row_inside < col_inside, 1, 0)
    for step, first, count in lists:
        def make(i, carry, step=step, first=first):
            col, _, rowwise, _ = piece(x, chip, step, i, nx, half_tiles, half_x)
            a_hi, a_lo = zhi[step], zlo[step]
            b_hi = chi[pl.ds(2 * col, 2)].reshape(2 * rows, width)
            b_lo = clo[pl.ds(2 * col, 2)].reshape(2 * rows, width)

            @pl.when(rowwise)
            def _():
                full = mul(a_hi, a_lo, b_hi, b_lo)
                if step == 0:
                    full = jnp.where(above * jnp.where(i == 0, 1, 0) == 1, 0.0, full)
                pieces[first + i, 0] = full[:, :rows]
                pieces[first + i, 1] = full[:, rows:]

            @pl.when(jnp.logical_not(rowwise))
            def _():
                full = mul(b_hi, b_lo, a_hi, a_lo)
                pieces[first + i, 0] = full[:rows]
                pieces[first + i, 1] = full[rows:]

            return carry
        lax.fori_loop(0, count, make, 0)

    def arrival(offset):
        return pl.ds(offset * capacity * 2, capacity * 2)

    def exchange(offset):
        dest = lax.rem(y + offset, ny)
        send(
            outgoing.at[offset], incoming.at[arrival(offset)],
            xs.at[offset], xr.at[offset], (x, dest),
        )

    order = [o for o in range(1, ny)]
    for n, offset in enumerate(order):
        for k in range(capacity):
            outgoing[offset, 2 * k:2 * k + 2] = pieces[chosen[offset][k]]
        if n > 0:
            exchange(order[n - 1])
    for k in range(capacity):
        incoming[2 * k:2 * k + 2] = pieces[chosen[0][k]]
    exchange(order[-1])
    for offset in range(1, ny):
        wait_recv(incoming.at[arrival(offset)], xr.at[offset])

    for s in range(slots):
        code = found[s]
        there = code >= 0
        safe = jnp.maximum(code, 0)
        rowwise = lax.rem(safe, 2) == 1
        rank = lax.rem(safe // 2, capacity)
        first_source = 2 * (safe // (2 * capacity))
        bases = [
            (lax.rem(y - first_source - h + ny, ny) * capacity + rank) * 2 for h in (0, 1)
        ]
        for i in (0, 1):
            for j in (0, 1):
                place_of = jnp.where(rowwise, bases[i] + j, bases[j] + i)
                value = incoming[place_of]
                out_ref[s, i * rows:(i + 1) * rows, j * rows:(j + 1) * rows] = jnp.where(
                    there, value, 0.0
                )
    for copy in started:
        copy.wait_send()


def per_device(mesh_shape, matrix_rows, tile_owner, tile_slot):
    nx, ny = mesh_shape
    rows, width = matrix_rows.shape
    half_tiles, half_x = ny // 2, nx // 2
    capacity = nx // 4 + 1
    slots = -(-tile_owner.shape[0] // (nx * ny))
    _, piece_count = piece_lists(half_tiles, half_x)
    reach = max(ny // 4, 1)
    f32, bf16 = jnp.float32, jnp.bfloat16
    dma = pltpu.SemaphoreType.DMA
    return pl.pallas_call(
        functools.partial(kernel, (nx, ny, half_tiles, half_x, capacity, slots)),
        out_shape=jax.ShapeDtypeStruct((slots, 2 * rows, 2 * rows), f32),
        in_specs=[
            pl.BlockSpec(memory_space=pltpu.VMEM),
            pl.BlockSpec(memory_space=pltpu.SMEM),
            pl.BlockSpec(memory_space=pltpu.SMEM),
        ],
        out_specs=pl.BlockSpec(memory_space=pltpu.VMEM),
        scratch_shapes=[
            pltpu.VMEM((ny, rows, width), f32),
            pltpu.VMEM((half_x, rows, width), f32),
            pltpu.VMEM((ny, rows, width), bf16),
            pltpu.VMEM((ny, rows, width), bf16),
            pltpu.VMEM((half_x + 1, rows, width), bf16),
            pltpu.VMEM((half_x + 1, rows, width), bf16),
            pltpu.VMEM((piece_count, 2, rows, rows), f32),
            pltpu.VMEM((ny, 2 * capacity, rows, rows), f32),
            pltpu.VMEM((ny * 2 * capacity, rows, rows), f32),
            pltpu.SMEM((piece_count,), jnp.int32),
            dma((reach, 2)), dma((reach, 2)), dma((reach, 2)), dma((reach, 2)),
            dma((2 * reach + 1, 2)), dma((2 * reach + 1, 2)),
            dma((half_x, 2)), dma((half_x, 2)),
            dma((ny,)), dma((ny,)),
        ],
        compiler_params=pltpu.CompilerParams(
            collective_id=0, has_side_effects=True, vmem_limit_bytes=60 * 1024 * 1024
        ),
    )(matrix_rows, tile_owner, tile_slot)


def solution(mesh):
    placed = (P(("gx", "gy"), None), P(), P())
    return jax.shard_map(
        functools.partial(per_device, (mesh.shape["gx"], mesh.shape["gy"])),
        mesh=mesh,
        in_specs=placed,
        out_specs=P(("gx", "gy"), None, None),
        check_vma=False,
    )
```

```python
import functools

import jax
import jax.numpy as jnp
from jax import lax
from jax.experimental import pallas as pl
from jax.experimental.pallas import tpu as pltpu
from jax.sharding import PartitionSpec as P

MESH = pl.DeviceIdType.MESH


def chip_position(chip, chips):
    row, col = lax.div(chip, 2), lax.rem(chip, 2)
    return col * (1 + row) + (1 - col) * lax.rem(chips - row, chips)


def chip_at(position, chips):
    behind = lax.rem(position + chips - 1, chips)
    far = lax.div(behind, chips // 2)
    return (1 - far) * (2 * behind + 1) + far * 2 * (chips - 1 - behind)


def piece_lists(half_tiles, half_x):
    lists, start = [], 0
    for step in range(half_x + 1):
        if step == 0:
            count = half_tiles // 2 + 1
        elif step < half_x:
            count = half_tiles
        else:
            count = half_tiles // 2
        lists.append((step, start, count))
        start += count
    return lists, start


def piece(x, r, step, i, nx, half_tiles, half_x):
    source = lax.rem(x - step + nx, nx)
    if step == 0:
        col = lax.rem(r - i + half_tiles, half_tiles)
        valid = jnp.logical_or(i < half_tiles // 2, r < half_tiles // 2)
        rowwise = col <= r
    elif step < half_x:
        col = i
        valid = i >= 0
        rowwise = source > x
    else:
        flag = jnp.where(x >= half_x, 1, 0)
        col = 2 * i + lax.rem(r + flag, 2)
        valid = i >= 0
        rowwise = source > x
    other, mine = source * half_tiles + r, x * half_tiles + col
    row_tile = jnp.where(rowwise, other, mine)
    col_tile = jnp.where(rowwise, mine, other)
    tile = jnp.where(valid, row_tile * (row_tile + 1) // 2 + col_tile, 0)
    return col, valid, rowwise, tile


def kernel(
    dims, rows_ref, owner_ref, slot_ref, out_ref,
    gath, zbuf, chi, clo, zsplit, pieces, outgoing, incoming, targets,
    gs_r, gr_r, gs_l, gr_l, ss, sr, zs, zr, xs, xr,
):
    nx, ny, half_tiles, half_x, capacity, slots = dims
    rows = rows_ref.shape[0]
    half = rows // 2
    chips = ny // 2
    reach = chips // 2
    x = lax.axis_index("gx")
    y = lax.axis_index("gy")
    core = lax.rem(y, 2)
    chip = lax.div(y, 2)
    right_x, left_x = lax.rem(x + 1, nx), lax.rem(x + nx - 1, nx)
    sibling = y + 1 - 2 * core
    place = chip_position(chip, chips)

    def at(position):
        return 2 * chip_at(lax.rem(position + chips, chips), chips) + core

    next_y, prev_y = at(place + 1), at(place - 1)
    lists, piece_count = piece_lists(half_tiles, half_x)

    barrier = pltpu.get_barrier_semaphore()
    for other in (right_x, left_x):
        pl.semaphore_signal(barrier, inc=1, device_id=(other, y), device_id_type=MESH)
    for offset in range(1, ny):
        pl.semaphore_signal(
            barrier, inc=1, device_id=(x, lax.rem(y + offset, ny)), device_id_type=MESH
        )
    pl.semaphore_wait(barrier, ny + 1)

    started = []

    def send(src, dst, send_sem, recv_sem, target):
        copy = pltpu.make_async_remote_copy(
            src_ref=src, dst_ref=dst, send_sem=send_sem, recv_sem=recv_sem,
            device_id=target, device_id_type=MESH,
        )
        copy.start()
        started.append(copy)

    def part(h):
        return pl.ds(h * half, half)

    def zcopy(step, h):
        src = rows_ref.at[part(h)] if step == 1 else zbuf.at[step - 2, part(h)]
        send(src, zbuf.at[step - 1, part(h)], zs.at[step - 1, h], zr.at[step - 1, h], (right_x, y))

    def block(owner, h):
        return gath.at[owner, part(h)]

    def ring(direction, distance, h):
        owner = at(place - direction * (distance - 1))
        src = rows_ref.at[part(h)] if distance == 1 else block(owner, h)
        s, r = (gs_r, gr_r) if direction == 1 else (gs_l, gr_l)
        target = next_y if direction == 1 else prev_y
        send(src, block(owner, h), s.at[distance - 1, h], r.at[distance - 1, h], (x, target))

    def cross(number, owner, h):
        src = rows_ref.at[part(h)] if number == 0 else block(owner, h)
        send(src, block(owner, h), ss.at[number, h], sr.at[number, h], (x, sibling))

    def halves_of(direction, distance):
        if distance < reach:
            return (0, 1) if direction == 1 else (1, 0)
        return (0,) if direction == 1 else (1,)

    def split(value, hi_ref, lo_ref, index):
        hi = value.astype(jnp.bfloat16)
        hi_ref[index] = hi
        lo_ref[index] = (value - hi.astype(jnp.float32)).astype(jnp.bfloat16)

    zcopy(1, 0)
    ring(1, 1, 0)
    if reach > 1:
        ring(-1, 1, 1)
        zcopy(1, 1)
        ring(1, 1, 1)
        ring(-1, 1, 0)
    else:
        ring(-1, 1, 1)
        zcopy(1, 1)
    cross(0, y, 0)
    cross(0, y, 1)

    for step, first, count in lists:
        def fill(i, carry, step=step, first=first):
            _, valid, _, tile = piece(x, chip, step, i, nx, half_tiles, half_x)
            targets[first + i] = jnp.where(valid, lax.rem(owner_ref[tile], ny), ny)
            return carry
        lax.fori_loop(0, count, fill, 0)

    me = x * ny + y

    def class_loop(r, carry):
        state = (jnp.int32(0),) + carry
        for step, first, count in lists:
            def look(i, state, step=step):
                seen, found = state[0], state[1:]
                _, valid, rowwise, tile = piece(x, r, step, i, nx, half_tiles, half_x)
                mine = jnp.where(valid, jnp.where(owner_ref[tile] == me, 1, 0), 0)
                slot = slot_ref[tile]
                code = 2 * (r * capacity + jnp.minimum(seen, capacity - 1))
                code = code + jnp.where(rowwise, 1, 0)
                key = jnp.where(mine == 1, slot, slots)
                found = tuple(jnp.where(key == s, code, found[s]) for s in range(slots))
                return (seen + mine,) + found
            state = lax.fori_loop(0, count, look, state)
        return state[1:]

    found = lax.fori_loop(0, half_tiles, class_loop, (jnp.int32(-1),) * slots)

    chosen = []
    for offset in range(ny):
        dest = lax.rem(y + offset, ny)

        def pick(p, state, dest=dest):
            hit = jnp.where(targets[p] == dest, 1, 0)
            seen = state[0]
            key = jnp.where(hit == 1, seen, capacity)
            picks = tuple(jnp.where(key == k, p, state[1 + k]) for k in range(capacity))
            return (seen + hit,) + picks

        chosen.append(lax.fori_loop(0, piece_count, pick, (jnp.int32(0),) * (capacity + 1))[1:])

    def wait_recv(dst, sem):
        pltpu.make_async_remote_copy(
            src_ref=dst, dst_ref=dst, send_sem=sem, recv_sem=sem,
            device_id=(x, sibling), device_id_type=MESH,
        ).wait_recv()

    def split_other(step, h):
        ref = rows_ref.at[part(h)] if step == 0 else zbuf.at[step - 1, part(h)]
        value = ref[...]
        hi = value.astype(jnp.bfloat16)
        zsplit[step, h, :half] = hi
        zsplit[step, h, half:] = (value - hi.astype(jnp.float32)).astype(jnp.bfloat16)

    def take_other(step, h):
        wait_recv(zbuf.at[step - 1, part(h)], zr.at[step - 1, h])
        if step < half_x:
            zcopy(step + 1, h)

    split_other(0, 0)
    split_other(0, 1)
    split(rows_ref[...], chi, clo, y)

    def take_cross(number, owner, halves):
        for h in halves:
            wait_recv(block(owner, h), sr.at[number, h])

    number = 1
    pending = [(0, sibling, (0, 1))]
    for distance in range(1, reach + 1):
        if distance <= half_x:
            for h in (0, 1):
                if (distance, h) != (half_x, 1):
                    take_other(distance, h)
                if h in halves_of(1, distance):
                    owner = at(place - distance)
                    wait_recv(block(owner, h), gr_r.at[distance - 1, h])
                    if distance < reach and h in halves_of(1, distance + 1):
                        ring(1, distance + 1, h)
                    cross(2 * distance - 1, owner, h)
                g = 1 - h
                if g in halves_of(-1, distance):
                    owner = at(place + distance)
                    wait_recv(block(owner, g), gr_l.at[distance - 1, g])
                    if distance < reach and g in halves_of(-1, distance + 1):
                        ring(-1, distance + 1, g)
                    cross(2 * distance, owner, g)
            split_other(distance, 0)
            if distance < half_x:
                split_other(distance, 1)
        behind, ahead = at(place - distance), at(place + distance)
        pending.append((2 * distance - 1, behind + 1 - 2 * core, halves_of(1, distance)))
        pending.append((2 * distance, ahead + 1 - 2 * core, halves_of(-1, distance)))
        split(gath[behind], chi, clo, behind)
        if distance < reach:
            split(gath[ahead], chi, clo, ahead)
        for number, owner, halves in pending[: (1 if distance == 1 else 0)]:
            take_cross(number, owner, halves)
            split(gath[owner], chi, clo, owner)
    for number, owner, halves in pending[1:-2]:
        take_cross(number, owner, halves)
        split(gath[owner], chi, clo, owner)
    for number, owner, halves in pending[-2:]:
        take_cross(number, owner, halves)
    split(gath[pending[-1][1]], chi, clo, pending[-1][1])
    for step in range(reach + 1, half_x + 1):
        for h in (0, 1):
            if (step, h) != (half_x, 1):
                take_other(step, h)
                split_other(step, h)

    one = functools.partial(
        lax.dot_general,
        dimension_numbers=(((1,), (1,)), ((), ())),
        preferred_element_type=jnp.float32,
    )
    width = rows_ref.shape[1]
    row_inside = core * rows + lax.broadcasted_iota(jnp.int32, (half, 2 * rows), 0)
    col_inside = lax.broadcasted_iota(jnp.int32, (half, 2 * rows), 1)

    def multiply(h):
        above = jnp.where(row_inside + h * half < col_inside, 1, 0)
        for step, first, count in lists:
            def make(i, carry, step=step, first=first):
                col, _, _, _ = piece(x, chip, step, i, nx, half_tiles, half_x)
                b_hi = chi[pl.ds(2 * col, 2)].reshape(2 * rows, width)
                b_lo = clo[pl.ds(2 * col, 2)].reshape(2 * rows, width)
                both = one(zsplit[step, h], b_hi)
                full = both[:half] + (both[half:] + one(zsplit[step, h, :half], b_lo))
                if step == 0:
                    full = jnp.where(above * jnp.where(i == 0, 1, 0) == 1, 0.0, full)
                pieces[h, first + i, 0] = full[:, :rows]
                pieces[h, first + i, 1] = full[:, rows:]
                return carry
            lax.fori_loop(0, count, make, 0)

    def arrival(offset):
        return pl.ds(offset * capacity * 2, capacity * 2)

    def exchange(h, offset):
        send(
            outgoing.at[h, offset], incoming.at[h, arrival(offset)],
            xs.at[h, offset], xr.at[h, offset], (x, lax.rem(y + offset, ny)),
        )

    for h in (0, 1):
        if h == 1:
            take_other(half_x, 1)
            split_other(half_x, 1)
        multiply(h)
        for offset in range(1, ny):
            for k in range(capacity):
                outgoing[h, offset, 2 * k:2 * k + 2] = pieces[h, chosen[offset][k]]
            if offset > 1:
                exchange(h, offset - 1)
        for k in range(capacity):
            incoming[h, 2 * k:2 * k + 2] = pieces[h, chosen[0][k]]
        exchange(h, ny - 1)
    for h in (0, 1):
        for offset in range(1, ny):
            wait_recv(incoming.at[h, arrival(offset)], xr.at[h, offset])

    for s in range(slots):
        code = found[s]
        there = code >= 0
        safe = jnp.maximum(code, 0)
        rowwise = lax.rem(safe, 2) == 1
        rank = lax.rem(safe // 2, capacity)
        first_source = 2 * (safe // (2 * capacity))
        bases = [
            (lax.rem(y - first_source - h + ny, ny) * capacity + rank) * 2 for h in (0, 1)
        ]
        for i in (0, 1):
            for j in (0, 1):
                place_of = jnp.where(rowwise, bases[i] + j, bases[j] + i)
                value = jnp.concatenate([incoming[0, place_of], incoming[1, place_of]], axis=0)
                value = jnp.where(rowwise, value, value.T)
                out_ref[s, i * rows:(i + 1) * rows, j * rows:(j + 1) * rows] = jnp.where(
                    there, value, 0.0
                )
    for copy in started:
        copy.wait_send()


def per_device(mesh_shape, matrix_rows, tile_owner, tile_slot):
    nx, ny = mesh_shape
    rows, width = matrix_rows.shape
    half_tiles, half_x = ny // 2, nx // 2
    capacity = nx // 4 + 1
    slots = -(-tile_owner.shape[0] // (nx * ny))
    _, piece_count = piece_lists(half_tiles, half_x)
    reach = max(ny // 4, 1)
    f32, bf16 = jnp.float32, jnp.bfloat16
    dma = pltpu.SemaphoreType.DMA
    return pl.pallas_call(
        functools.partial(kernel, (nx, ny, half_tiles, half_x, capacity, slots)),
        out_shape=jax.ShapeDtypeStruct((slots, 2 * rows, 2 * rows), f32),
        in_specs=[
            pl.BlockSpec(memory_space=pltpu.VMEM),
            pl.BlockSpec(memory_space=pltpu.SMEM),
            pl.BlockSpec(memory_space=pltpu.SMEM),
        ],
        out_specs=pl.BlockSpec(memory_space=pltpu.VMEM),
        scratch_shapes=[
            pltpu.VMEM((ny, rows, width), f32),
            pltpu.VMEM((half_x, rows, width), f32),
            pltpu.VMEM((ny, rows, width), bf16),
            pltpu.VMEM((ny, rows, width), bf16),
            pltpu.VMEM((half_x + 1, 2, rows, width), bf16),
            pltpu.VMEM((2, piece_count, 2, rows // 2, rows), f32),
            pltpu.VMEM((2, ny, 2 * capacity, rows // 2, rows), f32),
            pltpu.VMEM((2, ny * 2 * capacity, rows // 2, rows), f32),
            pltpu.SMEM((piece_count,), jnp.int32),
            dma((reach, 2)), dma((reach, 2)), dma((reach, 2)), dma((reach, 2)),
            dma((2 * reach + 1, 2)), dma((2 * reach + 1, 2)),
            dma((half_x, 2)), dma((half_x, 2)),
            dma((2, ny)), dma((2, ny)),
        ],
        compiler_params=pltpu.CompilerParams(
            collective_id=0, has_side_effects=True, vmem_limit_bytes=60 * 1024 * 1024
        ),
    )(matrix_rows, tile_owner, tile_slot)


def solution(mesh):
    placed = (P(("gx", "gy"), None), P(), P())
    return jax.shard_map(
        functools.partial(per_device, (mesh.shape["gx"], mesh.shape["gy"])),
        mesh=mesh,
        in_specs=placed,
        out_specs=P(("gx", "gy"), None, None),
        check_vma=False,
    )
```

```python
import functools

import jax
import jax.numpy as jnp
from jax import lax
from jax.experimental import pallas as pl
from jax.experimental.pallas import tpu as pltpu
from jax.sharding import PartitionSpec as P

MESH = pl.DeviceIdType.MESH


def chip_position(chip, chips):
    row, col = lax.div(chip, 2), lax.rem(chip, 2)
    return col * (1 + row) + (1 - col) * lax.rem(chips - row, chips)


def chip_at(position, chips):
    behind = lax.rem(position + chips - 1, chips)
    far = lax.div(behind, chips // 2)
    return (1 - far) * (2 * behind + 1) + far * 2 * (chips - 1 - behind)


def piece_lists(half_tiles, half_x):
    lists, start = [], 0
    for step in range(half_x + 1):
        if step == 0:
            count = half_tiles // 2 + 1
        elif step < half_x:
            count = half_tiles
        else:
            count = half_tiles // 2
        lists.append((step, start, count))
        start += count
    return lists, start


def piece(x, r, step, i, nx, half_tiles, half_x):
    source = lax.rem(x - step + nx, nx)
    if step == 0:
        col = lax.rem(r - i + half_tiles, half_tiles)
        valid = jnp.logical_or(i < half_tiles // 2, r < half_tiles // 2)
        rowwise = col <= r
    elif step < half_x:
        col = i
        valid = i >= 0
        rowwise = source > x
    else:
        flag = jnp.where(x >= half_x, 1, 0)
        col = 2 * i + lax.rem(r + flag, 2)
        valid = i >= 0
        rowwise = source > x
    other, mine = source * half_tiles + r, x * half_tiles + col
    row_tile = jnp.where(rowwise, other, mine)
    col_tile = jnp.where(rowwise, mine, other)
    tile = jnp.where(valid, row_tile * (row_tile + 1) // 2 + col_tile, 0)
    return col, valid, rowwise, tile


def kernel(
    dims, rows_ref, owner_ref, slot_ref, out_ref,
    gath, zbuf, chi, clo, zsplit, pieces, outgoing, incoming, targets,
    gs_r, gr_r, gs_l, gr_l, ss, sr, zs, zr, xs, xr,
):
    nx, ny, half_tiles, half_x, capacity, slots = dims
    rows = rows_ref.shape[0]
    half = rows // 2
    chips = ny // 2
    reach = chips // 2
    x = lax.axis_index("gx")
    y = lax.axis_index("gy")
    core = lax.rem(y, 2)
    chip = lax.div(y, 2)
    right_x, left_x = lax.rem(x + 1, nx), lax.rem(x + nx - 1, nx)
    sibling = y + 1 - 2 * core
    place = chip_position(chip, chips)

    def at(position):
        return 2 * chip_at(lax.rem(position + chips, chips), chips) + core

    next_y, prev_y = at(place + 1), at(place - 1)
    lists, piece_count = piece_lists(half_tiles, half_x)

    barrier = pltpu.get_barrier_semaphore()
    for other in (right_x, left_x):
        pl.semaphore_signal(barrier, inc=1, device_id=(other, y), device_id_type=MESH)
    for offset in range(1, ny):
        pl.semaphore_signal(
            barrier, inc=1, device_id=(x, lax.rem(y + offset, ny)), device_id_type=MESH
        )
    pl.semaphore_wait(barrier, ny + 1)

    started = []

    def send(src, dst, send_sem, recv_sem, target):
        copy = pltpu.make_async_remote_copy(
            src_ref=src, dst_ref=dst, send_sem=send_sem, recv_sem=recv_sem,
            device_id=target, device_id_type=MESH,
        )
        copy.start()
        started.append(copy)

    def part(h):
        return pl.ds(h * half, half)

    def zcopy(step, h):
        src = rows_ref.at[part(h)] if step == 1 else zbuf.at[step - 2, part(h)]
        send(src, zbuf.at[step - 1, part(h)], zs.at[step - 1, h], zr.at[step - 1, h], (right_x, y))

    def block(owner, h):
        return gath.at[owner, part(h)]

    def ring(direction, distance, h):
        owner = at(place - direction * (distance - 1))
        src = rows_ref.at[part(h)] if distance == 1 else block(owner, h)
        s, r = (gs_r, gr_r) if direction == 1 else (gs_l, gr_l)
        target = next_y if direction == 1 else prev_y
        send(src, block(owner, h), s.at[distance - 1, h], r.at[distance - 1, h], (x, target))

    def cross(number, owner, h):
        src = rows_ref.at[part(h)] if number == 0 else block(owner, h)
        send(src, block(owner, h), ss.at[number, h], sr.at[number, h], (x, sibling))

    def halves_of(direction, distance):
        if distance < reach:
            return (0, 1) if direction == 1 else (1, 0)
        return (0,) if direction == 1 else (1,)

    def split(value, hi_ref, lo_ref, index):
        hi = value.astype(jnp.bfloat16)
        hi_ref[index] = hi
        lo_ref[index] = (value - hi.astype(jnp.float32)).astype(jnp.bfloat16)

    zcopy(1, 0)
    ring(1, 1, 0)
    if reach > 1:
        ring(-1, 1, 1)
        zcopy(1, 1)
        ring(1, 1, 1)
        ring(-1, 1, 0)
    else:
        ring(-1, 1, 1)
        zcopy(1, 1)
    cross(0, y, 0)
    cross(0, y, 1)

    for step, first, count in lists:
        def fill(i, carry, step=step, first=first):
            _, valid, _, tile = piece(x, chip, step, i, nx, half_tiles, half_x)
            targets[first + i] = jnp.where(valid, lax.rem(owner_ref[tile], ny), ny)
            return carry
        lax.fori_loop(0, count, fill, 0)

    me = x * ny + y

    def class_loop(r, carry):
        state = (jnp.int32(0),) + carry
        for step, first, count in lists:
            def look(i, state, step=step):
                seen, found = state[0], state[1:]
                _, valid, rowwise, tile = piece(x, r, step, i, nx, half_tiles, half_x)
                mine = jnp.where(valid, jnp.where(owner_ref[tile] == me, 1, 0), 0)
                slot = slot_ref[tile]
                code = 2 * (r * capacity + jnp.minimum(seen, capacity - 1))
                code = code + jnp.where(rowwise, 1, 0)
                key = jnp.where(mine == 1, slot, slots)
                found = tuple(jnp.where(key == s, code, found[s]) for s in range(slots))
                return (seen + mine,) + found
            state = lax.fori_loop(0, count, look, state)
        return state[1:]

    found = lax.fori_loop(0, half_tiles, class_loop, (jnp.int32(-1),) * slots)

    chosen = []
    for offset in range(ny):
        dest = lax.rem(y + offset, ny)

        def pick(p, state, dest=dest):
            hit = jnp.where(targets[p] == dest, 1, 0)
            seen = state[0]
            key = jnp.where(hit == 1, seen, capacity)
            picks = tuple(jnp.where(key == k, p, state[1 + k]) for k in range(capacity))
            return (seen + hit,) + picks

        chosen.append(lax.fori_loop(0, piece_count, pick, (jnp.int32(0),) * (capacity + 1))[1:])

    def wait_recv(dst, sem):
        pltpu.make_async_remote_copy(
            src_ref=dst, dst_ref=dst, send_sem=sem, recv_sem=sem,
            device_id=(x, sibling), device_id_type=MESH,
        ).wait_recv()

    def split_other(step, h):
        ref = rows_ref.at[part(h)] if step == 0 else zbuf.at[step - 1, part(h)]
        value = ref[...]
        hi = value.astype(jnp.bfloat16)
        zsplit[step, h, :half] = hi
        zsplit[step, h, half:] = (value - hi.astype(jnp.float32)).astype(jnp.bfloat16)

    def take_other(step, h):
        wait_recv(zbuf.at[step - 1, part(h)], zr.at[step - 1, h])
        if step < half_x:
            zcopy(step + 1, h)

    split_other(0, 0)
    split_other(0, 1)
    split(rows_ref[...], chi, clo, y)

    def take_cross(number, owner, halves):
        for h in halves:
            wait_recv(block(owner, h), sr.at[number, h])

    one = functools.partial(
        lax.dot_general,
        dimension_numbers=(((1,), (1,)), ((), ())),
        preferred_element_type=jnp.float32,
    )
    width = rows_ref.shape[1]
    row_inside = core * rows + lax.broadcasted_iota(jnp.int32, (half, 2 * rows), 0)
    col_inside = lax.broadcasted_iota(jnp.int32, (half, 2 * rows), 1)

    def one_piece_of(h):
        above = jnp.where(row_inside + h * half < col_inside, 1, 0)

        def one_piece(i, step, first, col):
            b_hi = chi[pl.ds(2 * col, 2)].reshape(2 * rows, width)
            b_lo = clo[pl.ds(2 * col, 2)].reshape(2 * rows, width)
            both = one(zsplit[step, h], b_hi)
            full = both[:half] + (both[half:] + one(zsplit[step, h, :half], b_lo))
            if step == 0:
                full = jnp.where(above * jnp.where(i == 0, 1, 0) == 1, 0.0, full)
            pieces[h, first + i, 0] = full[:, :rows]
            pieces[h, first + i, 1] = full[:, rows:]

        return one_piece

    farthest = chip_at(lax.rem(place + reach, chips), chips)
    soon = min(reach, half_x) if reach > 1 else 0

    def multiply(h, mode):
        one_piece = one_piece_of(h)
        for step, first, count in lists:
            if mode == "early" and step >= soon:
                continue

            def make(i, carry, step=step, first=first):
                col, _, _, _ = piece(x, chip, step, i, nx, half_tiles, half_x)
                if mode == "all" or step >= soon:
                    one_piece(i, step, first, col)
                else:
                    wanted = (col != farthest) if mode == "early" else (col == farthest)
                    pl.when(wanted)(lambda: one_piece(i, step, first, col))
                return carry
            lax.fori_loop(0, count, make, 0)

    pending = [(0, sibling, (0, 1))]
    for distance in range(1, reach + 1):
        if distance == reach:
            for number, owner, halves in pending[1:]:
                take_cross(number, owner, halves)
                split(gath[owner], chi, clo, owner)
            multiply(0, "early")
        if distance <= half_x:
            for h in (0, 1):
                if (distance, h) != (half_x, 1):
                    take_other(distance, h)
                if h in halves_of(1, distance):
                    owner = at(place - distance)
                    wait_recv(block(owner, h), gr_r.at[distance - 1, h])
                    if distance < reach and h in halves_of(1, distance + 1):
                        ring(1, distance + 1, h)
                    cross(2 * distance - 1, owner, h)
                g = 1 - h
                if g in halves_of(-1, distance):
                    owner = at(place + distance)
                    wait_recv(block(owner, g), gr_l.at[distance - 1, g])
                    if distance < reach and g in halves_of(-1, distance + 1):
                        ring(-1, distance + 1, g)
                    cross(2 * distance, owner, g)
            split_other(distance, 0)
            if distance < half_x:
                split_other(distance, 1)
        behind, ahead = at(place - distance), at(place + distance)
        pending.append((2 * distance - 1, behind + 1 - 2 * core, halves_of(1, distance)))
        pending.append((2 * distance, ahead + 1 - 2 * core, halves_of(-1, distance)))
        split(gath[behind], chi, clo, behind)
        if distance < reach:
            split(gath[ahead], chi, clo, ahead)
        for number, owner, halves in pending[: (1 if distance == 1 else 0)]:
            take_cross(number, owner, halves)
            split(gath[owner], chi, clo, owner)
    for number, owner, halves in pending[-2:]:
        take_cross(number, owner, halves)
    split(gath[pending[-1][1]], chi, clo, pending[-1][1])
    for step in range(reach + 1, half_x + 1):
        for h in (0, 1):
            if (step, h) != (half_x, 1):
                take_other(step, h)
                split_other(step, h)

    def arrival(offset):
        return pl.ds(offset * capacity * 2, capacity * 2)

    def exchange(h, offset):
        send(
            outgoing.at[h, offset], incoming.at[h, arrival(offset)],
            xs.at[h, offset], xr.at[h, offset], (x, lax.rem(y + offset, ny)),
        )

    for h in (0, 1):
        if h == 1:
            take_other(half_x, 1)
            split_other(half_x, 1)
        multiply(h, "all" if h == 1 else "late")
        for offset in range(1, ny):
            for k in range(capacity):
                outgoing[h, offset, 2 * k:2 * k + 2] = pieces[h, chosen[offset][k]]
            if offset > 1:
                exchange(h, offset - 1)
        for k in range(capacity):
            incoming[h, 2 * k:2 * k + 2] = pieces[h, chosen[0][k]]
        exchange(h, ny - 1)
    for h in (0, 1):
        for offset in range(1, ny):
            wait_recv(incoming.at[h, arrival(offset)], xr.at[h, offset])

    for s in range(slots):
        code = found[s]
        there = code >= 0
        safe = jnp.maximum(code, 0)
        rowwise = lax.rem(safe, 2) == 1
        rank = lax.rem(safe // 2, capacity)
        first_source = 2 * (safe // (2 * capacity))
        bases = [
            (lax.rem(y - first_source - h + ny, ny) * capacity + rank) * 2 for h in (0, 1)
        ]
        for i in (0, 1):
            for j in (0, 1):
                place_of = jnp.where(rowwise, bases[i] + j, bases[j] + i)
                value = jnp.concatenate([incoming[0, place_of], incoming[1, place_of]], axis=0)
                value = jnp.where(rowwise, value, value.T)
                out_ref[s, i * rows:(i + 1) * rows, j * rows:(j + 1) * rows] = jnp.where(
                    there, value, 0.0
                )
    for copy in started:
        copy.wait_send()


def per_device(mesh_shape, matrix_rows, tile_owner, tile_slot):
    nx, ny = mesh_shape
    rows, width = matrix_rows.shape
    half_tiles, half_x = ny // 2, nx // 2
    capacity = nx // 4 + 1
    slots = -(-tile_owner.shape[0] // (nx * ny))
    _, piece_count = piece_lists(half_tiles, half_x)
    reach = max(ny // 4, 1)
    f32, bf16 = jnp.float32, jnp.bfloat16
    dma = pltpu.SemaphoreType.DMA
    return pl.pallas_call(
        functools.partial(kernel, (nx, ny, half_tiles, half_x, capacity, slots)),
        out_shape=jax.ShapeDtypeStruct((slots, 2 * rows, 2 * rows), f32),
        in_specs=[
            pl.BlockSpec(memory_space=pltpu.VMEM),
            pl.BlockSpec(memory_space=pltpu.SMEM),
            pl.BlockSpec(memory_space=pltpu.SMEM),
        ],
        out_specs=pl.BlockSpec(memory_space=pltpu.VMEM),
        scratch_shapes=[
            pltpu.VMEM((ny, rows, width), f32),
            pltpu.VMEM((half_x, rows, width), f32),
            pltpu.VMEM((ny, rows, width), bf16),
            pltpu.VMEM((ny, rows, width), bf16),
            pltpu.VMEM((half_x + 1, 2, rows, width), bf16),
            pltpu.VMEM((2, piece_count, 2, rows // 2, rows), f32),
            pltpu.VMEM((2, ny, 2 * capacity, rows // 2, rows), f32),
            pltpu.VMEM((2, ny * 2 * capacity, rows // 2, rows), f32),
            pltpu.SMEM((piece_count,), jnp.int32),
            dma((reach, 2)), dma((reach, 2)), dma((reach, 2)), dma((reach, 2)),
            dma((2 * reach + 1, 2)), dma((2 * reach + 1, 2)),
            dma((half_x, 2)), dma((half_x, 2)),
            dma((2, ny)), dma((2, ny)),
        ],
        compiler_params=pltpu.CompilerParams(
            collective_id=0, has_side_effects=True, vmem_limit_bytes=60 * 1024 * 1024
        ),
    )(matrix_rows, tile_owner, tile_slot)


def solution(mesh):
    placed = (P(("gx", "gy"), None), P(), P())
    return jax.shard_map(
        functools.partial(per_device, (mesh.shape["gx"], mesh.shape["gy"])),
        mesh=mesh,
        in_specs=placed,
        out_specs=P(("gx", "gy"), None, None),
        check_vma=False,
    )
```

```python
import functools

import jax
import jax.numpy as jnp
from jax import lax
from jax.experimental import pallas as pl
from jax.experimental.pallas import tpu as pltpu
from jax.sharding import PartitionSpec as P

MESH = pl.DeviceIdType.MESH


def chip_position(chip, chips):
    row, col = lax.div(chip, 2), lax.rem(chip, 2)
    return col * (1 + row) + (1 - col) * lax.rem(chips - row, chips)


def chip_at(position, chips):
    behind = lax.rem(position + chips - 1, chips)
    far = lax.div(behind, chips // 2)
    return (1 - far) * (2 * behind + 1) + far * 2 * (chips - 1 - behind)


def piece_lists(half_tiles, half_x):
    lists, start = [], 0
    for step in range(half_x + 1):
        if step == 0:
            count = half_tiles // 2 + 1
        elif step < half_x:
            count = half_tiles
        else:
            count = half_tiles // 2
        lists.append((step, start, count))
        start += count
    return lists, start


def piece(x, r, step, i, nx, half_tiles, half_x):
    source = lax.rem(x - step + nx, nx)
    if step == 0:
        col = lax.rem(r - i + half_tiles, half_tiles)
        valid = jnp.logical_or(i < half_tiles // 2, r < half_tiles // 2)
        rowwise = col <= r
    elif step < half_x:
        col = i
        valid = i >= 0
        rowwise = source > x
    else:
        flag = jnp.where(x >= half_x, 1, 0)
        col = 2 * i + lax.rem(r + flag, 2)
        valid = i >= 0
        rowwise = source > x
    other, mine = source * half_tiles + r, x * half_tiles + col
    row_tile = jnp.where(rowwise, other, mine)
    col_tile = jnp.where(rowwise, mine, other)
    tile = jnp.where(valid, row_tile * (row_tile + 1) // 2 + col_tile, 0)
    return col, valid, rowwise, tile


def kernel(
    dims, rows_ref, owner_ref, slot_ref, out_ref,
    gath, zbuf, chi, clo, zsplit, pieces, outgoing, incoming, targets,
    gs_r, gr_r, gs_l, gr_l, ss, sr, zs, zr, xs, xr,
):
    nx, ny, half_tiles, half_x, capacity, slots = dims
    rows = rows_ref.shape[0]
    half = rows // 2
    chips = ny // 2
    reach = chips // 2
    x = lax.axis_index("gx")
    y = lax.axis_index("gy")
    core = lax.rem(y, 2)
    chip = lax.div(y, 2)
    right_x, left_x = lax.rem(x + 1, nx), lax.rem(x + nx - 1, nx)
    sibling = y + 1 - 2 * core
    place = chip_position(chip, chips)

    def at(position):
        return 2 * chip_at(lax.rem(position + chips, chips), chips) + core

    next_y, prev_y = at(place + 1), at(place - 1)
    lists, piece_count = piece_lists(half_tiles, half_x)

    barrier = pltpu.get_barrier_semaphore()
    for other in (right_x, left_x):
        pl.semaphore_signal(barrier, inc=1, device_id=(other, y), device_id_type=MESH)
    for offset in range(1, ny):
        pl.semaphore_signal(
            barrier, inc=1, device_id=(x, lax.rem(y + offset, ny)), device_id_type=MESH
        )
    pl.semaphore_wait(barrier, ny + 1)

    started = []

    def send(src, dst, send_sem, recv_sem, target):
        copy = pltpu.make_async_remote_copy(
            src_ref=src, dst_ref=dst, send_sem=send_sem, recv_sem=recv_sem,
            device_id=target, device_id_type=MESH,
        )
        copy.start()
        started.append(copy)

    def part(h):
        return pl.ds(h * half, half)

    def zcopy(step, h):
        src = rows_ref.at[part(h)] if step == 1 else zbuf.at[step - 2, part(h)]
        send(src, zbuf.at[step - 1, part(h)], zs.at[step - 1, h], zr.at[step - 1, h], (right_x, y))

    def block(owner, h):
        return gath.at[owner, part(h)]

    def ring(direction, distance, h):
        owner = at(place - direction * (distance - 1))
        src = rows_ref.at[part(h)] if distance == 1 else block(owner, h)
        s, r = (gs_r, gr_r) if direction == 1 else (gs_l, gr_l)
        target = next_y if direction == 1 else prev_y
        send(src, block(owner, h), s.at[distance - 1, h], r.at[distance - 1, h], (x, target))

    def cross(number, owner, h):
        src = rows_ref.at[part(h)] if number == 0 else block(owner, h)
        send(src, block(owner, h), ss.at[number, h], sr.at[number, h], (x, sibling))

    def halves_of(direction, distance):
        if distance < reach:
            return (0, 1) if direction == 1 else (1, 0)
        return (0,) if direction == 1 else (1,)

    def split(value, hi_ref, lo_ref, index):
        hi = value.astype(jnp.bfloat16)
        hi_ref[index] = hi
        lo_ref[index] = (value - hi.astype(jnp.float32)).astype(jnp.bfloat16)

    zcopy(1, 0)
    ring(1, 1, 0)
    if reach > 1:
        ring(-1, 1, 1)
        zcopy(1, 1)
        ring(1, 1, 1)
        ring(-1, 1, 0)
    else:
        ring(-1, 1, 1)
        zcopy(1, 1)
    cross(0, y, 0)
    cross(0, y, 1)

    for step, first, count in lists:
        def fill(i, carry, step=step, first=first):
            _, valid, _, tile = piece(x, chip, step, i, nx, half_tiles, half_x)
            targets[first + i] = jnp.where(valid, lax.rem(owner_ref[tile], ny), ny)
            return carry
        lax.fori_loop(0, count, fill, 0)

    me = x * ny + y

    def class_loop(r, carry):
        state = (jnp.int32(0),) + carry
        for step, first, count in lists:
            def look(i, state, step=step):
                seen, found = state[0], state[1:]
                _, valid, rowwise, tile = piece(x, r, step, i, nx, half_tiles, half_x)
                mine = jnp.where(valid, jnp.where(owner_ref[tile] == me, 1, 0), 0)
                slot = slot_ref[tile]
                code = 2 * (r * capacity + jnp.minimum(seen, capacity - 1))
                code = code + jnp.where(rowwise, 1, 0)
                key = jnp.where(mine == 1, slot, slots)
                found = tuple(jnp.where(key == s, code, found[s]) for s in range(slots))
                return (seen + mine,) + found
            state = lax.fori_loop(0, count, look, state)
        return state[1:]

    found = lax.fori_loop(0, half_tiles, class_loop, (jnp.int32(-1),) * slots)

    chosen = []
    for offset in range(ny):
        dest = lax.rem(y + offset, ny)

        def pick(p, state, dest=dest):
            hit = jnp.where(targets[p] == dest, 1, 0)
            seen = state[0]
            key = jnp.where(hit == 1, seen, capacity)
            picks = tuple(jnp.where(key == k, p, state[1 + k]) for k in range(capacity))
            return (seen + hit,) + picks

        chosen.append(lax.fori_loop(0, piece_count, pick, (jnp.int32(0),) * (capacity + 1))[1:])

    def wait_recv(dst, sem):
        pltpu.make_async_remote_copy(
            src_ref=dst, dst_ref=dst, send_sem=sem, recv_sem=sem,
            device_id=(x, sibling), device_id_type=MESH,
        ).wait_recv()

    def split_other(step, h):
        ref = rows_ref.at[part(h)] if step == 0 else zbuf.at[step - 1, part(h)]
        value = ref[...]
        hi = value.astype(jnp.bfloat16)
        zsplit[step, h, :half] = hi
        zsplit[step, h, half:] = (value - hi.astype(jnp.float32)).astype(jnp.bfloat16)

    def take_other(step, h):
        wait_recv(zbuf.at[step - 1, part(h)], zr.at[step - 1, h])
        if step < half_x:
            zcopy(step + 1, h)

    split_other(0, 0)
    split_other(0, 1)
    split(rows_ref[...], chi, clo, y)

    def take_cross(number, owner, halves):
        for h in halves:
            wait_recv(block(owner, h), sr.at[number, h])

    one = functools.partial(
        lax.dot_general,
        dimension_numbers=(((1,), (1,)), ((), ())),
        preferred_element_type=jnp.float32,
    )
    width = rows_ref.shape[1]
    row_inside = core * rows + lax.broadcasted_iota(jnp.int32, (half, 2 * rows), 0)
    col_inside = lax.broadcasted_iota(jnp.int32, (half, 2 * rows), 1)

    def one_piece_of(h):
        above = jnp.where(row_inside + h * half < col_inside, 1, 0)

        def one_piece(i, step, first, col):
            b_hi = chi[pl.ds(2 * col, 2)].reshape(2 * rows, width)
            b_lo = clo[pl.ds(2 * col, 2)].reshape(2 * rows, width)
            both = one(zsplit[step, h], b_hi)
            full = both[:half] + (both[half:] + one(zsplit[step, h, :half], b_lo))
            if step == 0:
                full = jnp.where(above * jnp.where(i == 0, 1, 0) == 1, 0.0, full)
            pieces[h, first + i, 0] = full[:, :rows]
            pieces[h, first + i, 1] = full[:, rows:]

        return one_piece

    farthest = chip_at(lax.rem(place + reach, chips), chips)
    soon = min(reach, half_x) if reach > 1 else 0

    def multiply(h, mode):
        one_piece = one_piece_of(h)
        for step, first, count in lists:
            if mode == "early" and step >= soon:
                continue
            if (mode == "before" and step == half_x) or (mode == "after" and step < half_x):
                continue

            def make(i, carry, step=step, first=first):
                col, _, _, _ = piece(x, chip, step, i, nx, half_tiles, half_x)
                if mode in ("before", "after") or step >= soon:
                    one_piece(i, step, first, col)
                else:
                    wanted = (col != farthest) if mode == "early" else (col == farthest)
                    pl.when(wanted)(lambda: one_piece(i, step, first, col))
                return carry
            lax.fori_loop(0, count, make, 0)

    pending = [(0, sibling, (0, 1))]
    for distance in range(1, reach + 1):
        if distance == reach:
            for number, owner, halves in pending[1:]:
                take_cross(number, owner, halves)
                split(gath[owner], chi, clo, owner)
            multiply(0, "early")
        if distance <= half_x:
            for h in (0, 1):
                if (distance, h) != (half_x, 1):
                    take_other(distance, h)
                if h in halves_of(1, distance):
                    owner = at(place - distance)
                    wait_recv(block(owner, h), gr_r.at[distance - 1, h])
                    if distance < reach and h in halves_of(1, distance + 1):
                        ring(1, distance + 1, h)
                    cross(2 * distance - 1, owner, h)
                g = 1 - h
                if g in halves_of(-1, distance):
                    owner = at(place + distance)
                    wait_recv(block(owner, g), gr_l.at[distance - 1, g])
                    if distance < reach and g in halves_of(-1, distance + 1):
                        ring(-1, distance + 1, g)
                    cross(2 * distance, owner, g)
            split_other(distance, 0)
            if distance < half_x:
                split_other(distance, 1)
        behind, ahead = at(place - distance), at(place + distance)
        pending.append((2 * distance - 1, behind + 1 - 2 * core, halves_of(1, distance)))
        pending.append((2 * distance, ahead + 1 - 2 * core, halves_of(-1, distance)))
        split(gath[behind], chi, clo, behind)
        if distance < reach:
            split(gath[ahead], chi, clo, ahead)
        for number, owner, halves in pending[: (1 if distance == 1 else 0)]:
            take_cross(number, owner, halves)
            split(gath[owner], chi, clo, owner)
    for number, owner, halves in pending[-2:]:
        take_cross(number, owner, halves)
    split(gath[pending[-1][1]], chi, clo, pending[-1][1])
    for step in range(reach + 1, half_x + 1):
        for h in (0, 1):
            if (step, h) != (half_x, 1):
                take_other(step, h)
                split_other(step, h)

    def arrival(offset):
        return pl.ds(offset * capacity * 2, capacity * 2)

    def exchange(h, offset):
        send(
            outgoing.at[h, offset], incoming.at[h, arrival(offset)],
            xs.at[h, offset], xr.at[h, offset], (x, lax.rem(y + offset, ny)),
        )

    for h in (0, 1):
        if h == 1:
            multiply(1, "before")
            take_other(half_x, 1)
            split_other(half_x, 1)
        multiply(h, "after" if h == 1 else "late")
        for offset in range(1, ny):
            for k in range(capacity):
                outgoing[h, offset, 2 * k:2 * k + 2] = pieces[h, chosen[offset][k]]
            if offset > 1:
                exchange(h, offset - 1)
        for k in range(capacity):
            incoming[h, 2 * k:2 * k + 2] = pieces[h, chosen[0][k]]
        exchange(h, ny - 1)
    for h in (0, 1):
        for offset in range(1, ny):
            wait_recv(incoming.at[h, arrival(offset)], xr.at[h, offset])

    for s in range(slots):
        code = found[s]
        there = code >= 0
        safe = jnp.maximum(code, 0)
        rowwise = lax.rem(safe, 2) == 1
        rank = lax.rem(safe // 2, capacity)
        first_source = 2 * (safe // (2 * capacity))
        bases = [
            (lax.rem(y - first_source - h + ny, ny) * capacity + rank) * 2 for h in (0, 1)
        ]
        for i in (0, 1):
            for j in (0, 1):
                place_of = jnp.where(rowwise, bases[i] + j, bases[j] + i)
                value = jnp.concatenate([incoming[0, place_of], incoming[1, place_of]], axis=0)
                value = jnp.where(rowwise, value, value.T)
                out_ref[s, i * rows:(i + 1) * rows, j * rows:(j + 1) * rows] = jnp.where(
                    there, value, 0.0
                )
    for copy in started:
        copy.wait_send()


def per_device(mesh_shape, matrix_rows, tile_owner, tile_slot):
    nx, ny = mesh_shape
    rows, width = matrix_rows.shape
    half_tiles, half_x = ny // 2, nx // 2
    capacity = nx // 4 + 1
    slots = -(-tile_owner.shape[0] // (nx * ny))
    _, piece_count = piece_lists(half_tiles, half_x)
    reach = max(ny // 4, 1)
    f32, bf16 = jnp.float32, jnp.bfloat16
    dma = pltpu.SemaphoreType.DMA
    return pl.pallas_call(
        functools.partial(kernel, (nx, ny, half_tiles, half_x, capacity, slots)),
        out_shape=jax.ShapeDtypeStruct((slots, 2 * rows, 2 * rows), f32),
        in_specs=[
            pl.BlockSpec(memory_space=pltpu.VMEM),
            pl.BlockSpec(memory_space=pltpu.SMEM),
            pl.BlockSpec(memory_space=pltpu.SMEM),
        ],
        out_specs=pl.BlockSpec(memory_space=pltpu.VMEM),
        scratch_shapes=[
            pltpu.VMEM((ny, rows, width), f32),
            pltpu.VMEM((half_x, rows, width), f32),
            pltpu.VMEM((ny, rows, width), bf16),
            pltpu.VMEM((ny, rows, width), bf16),
            pltpu.VMEM((half_x + 1, 2, rows, width), bf16),
            pltpu.VMEM((2, piece_count, 2, rows // 2, rows), f32),
            pltpu.VMEM((2, ny, 2 * capacity, rows // 2, rows), f32),
            pltpu.VMEM((2, ny * 2 * capacity, rows // 2, rows), f32),
            pltpu.SMEM((piece_count,), jnp.int32),
            dma((reach, 2)), dma((reach, 2)), dma((reach, 2)), dma((reach, 2)),
            dma((2 * reach + 1, 2)), dma((2 * reach + 1, 2)),
            dma((half_x, 2)), dma((half_x, 2)),
            dma((2, ny)), dma((2, ny)),
        ],
        compiler_params=pltpu.CompilerParams(
            collective_id=0, has_side_effects=True, vmem_limit_bytes=60 * 1024 * 1024
        ),
    )(matrix_rows, tile_owner, tile_slot)


def solution(mesh):
    placed = (P(("gx", "gy"), None), P(), P())
    return jax.shard_map(
        functools.partial(per_device, (mesh.shape["gx"], mesh.shape["gy"])),
        mesh=mesh,
        in_specs=placed,
        out_specs=P(("gx", "gy"), None, None),
        check_vma=False,
    )
```
